256 devices in a mesh: sa: 64 (over y_hi, z, x), ka: 2 (over y_lo), vert: 2 (over core).
Axes of the slice: x: 4, y: 4 (y_hi: 2, y_lo: 2; y = y_hi * 2 + y_lo), z: 8, core: 2. Of those that a mesh axis runs over, the one named last changes fastest.
Arguments:
- queries: bfloat16 [8192, 16, 128], P('sa', None, 'ka'), may hold values from -6 to 6
- key_rows: bfloat16 [8192, 16, 128], P('sa', None, 'ka'), may hold values from -6 to 6
- values: bfloat16 [8192, 16, 256], P('sa', None, 'vert'), may hold values from -6 to 6
- log_decays: bfloat16 [8192, 16, 128], P('sa', None, 'ka'), may hold values from -2 to 0
- output_grad: bfloat16 [8192, 16, 256], P('sa', None, 'vert'), may hold values from -0.0625 to 0.0625
Outputs:
- query_grad: float32 [8192, 16, 128], P('sa', 'vert', 'ka')
- key_grad: float32 [8192, 16, 128], P('sa', 'vert', 'ka')
- value_grad: float32 [8192, 16, 256], P('sa', 'ka', 'vert')
- decay_grad: float32 [8192, 16, 128], P('sa', 'vert', 'ka')
The draws below stay inside these ranges and needn't reach their ends.
All inputs are finite; a program needn't handle non-finite values.
Results may differ from the reference program's by a relative error of at most 0.0003.
Values may be sent and summed in bfloat16 or wider, within the bound.
A program may use at most 192 MiB of HBM per device.

```python
import math
import jax
import jax.numpy as jnp
from jax import lax

HEAD_NUMBER = 16
DK = 128
DV = 256
TILE_LEN = 64
TOK_DEV = 128
TOKEN_POSITIONS = 8192


def draw_log_decays(key, part):
    draw_keys = jax.random.split(jax.random.fold_in(key, 7), 7)
    slow_share = 0.5
    is_slow = jax.random.uniform(draw_keys[0], (HEAD_NUMBER, DK)) < slow_share
    slow_rate = jnp.exp(jax.random.uniform(draw_keys[1], (HEAD_NUMBER, DK), minval=math.log(0.15), maxval=math.log(0.45))) / TOKEN_POSITIONS
    fast_rate = math.log(10.0) / jnp.exp(jax.random.uniform(draw_keys[2], (HEAD_NUMBER, DK), minval=math.log(30.0), maxval=math.log(50.0)))
    step_rate = jnp.where(is_slow, slow_rate, fast_rate)
    block_count = TOKEN_POSITIONS // TOK_DEV
    block_factor = jnp.exp(jax.random.uniform(draw_keys[3], (block_count, 1, HEAD_NUMBER, 1), minval=math.log(0.5), maxval=math.log(2.0)))
    roughness = jax.random.uniform(draw_keys[4], (block_count, TOK_DEV, HEAD_NUMBER, DK), minval=0.4, maxval=1.6)
    logarithm_decay = -(step_rate[None, None] * block_factor * roughness).reshape(TOKEN_POSITIONS, HEAD_NUMBER, DK)
    spike_locations = jax.random.randint(draw_keys[5], (3,), 0, TOKEN_POSITIONS)
    spike_penalty = jnp.log(jax.random.uniform(draw_keys[6], (3, HEAD_NUMBER), minval=0.5, maxval=0.8))
    spike_matches = (jnp.arange(TOKEN_POSITIONS)[:, None] == spike_locations[None, :]).astype(jnp.float32)
    logarithm_decay = logarithm_decay + jnp.dot(spike_matches, spike_penalty)[:, :, None]
    return logarithm_decay.astype(jnp.bfloat16)


def block_levels(key, extent, shards, smallest, top_value):
    factor_of = 1.0
    for axis_at, parts in shards:
        draws = jax.random.uniform(jax.random.fold_in(jax.random.fold_in(key, 6), axis_at), (parts,), jnp.float32, smallest / len(shards), top_value / len(shards))
        factor_of = factor_of * jnp.repeat(jnp.exp(draws), extent[axis_at] // parts).reshape((-1,) + (1,) * (len(extent) - 1 - axis_at))
    return factor_of


def gaussian(own_key, shape, deviation, bound, cuts=(), kind=jnp.bfloat16):
    array = jax.random.normal(own_key, shape, jnp.float32) * deviation
    if len(cuts) > 0:
        array = block_levels(own_key, shape, cuts, -0.22, 0.18) * array
    return jnp.clip(array, min=-bound, max=bound).astype(kind)


def setup_inputs(seed: int = 0) -> dict:
    streams_of = jax.random.split(jax.random.key(seed), 6)
    queries = gaussian(streams_of[0], (TOKEN_POSITIONS, HEAD_NUMBER, DK), 1.0, 6.0, ((0, 64), (2, 2)))
    key_rows = gaussian(streams_of[1], (TOKEN_POSITIONS, HEAD_NUMBER, DK), 1.0, 6.0, ((0, 64), (2, 2)))
    values = gaussian(streams_of[2], (TOKEN_POSITIONS, HEAD_NUMBER, DV), 1.0, 6.0, ((0, 64), (2, 2)))
    log_decays = draw_log_decays(jax.random.fold_in(streams_of[5], 71), 0)
    output_grad = gaussian(streams_of[4], (TOKEN_POSITIONS, HEAD_NUMBER, DV), (6.0 / (DV * TOKEN_POSITIONS) ** 0.5), 0.0625, ((0, 64), (2, 2)))
    return {"queries": queries, "key_rows": key_rows, "values": values, "log_decays": log_decays, "output_grad": output_grad}


largest_entry = lax.Precision.HIGHEST


def to_blocks(tensor, length):
    row_count, head_count, channels = tensor.shape
    return tensor.astype(jnp.float32).reshape(row_count // length, length, head_count, channels).transpose(0, 2, 1, 3)


def from_blocks(tensor):
    tile_count, head_count, length, channels = tensor.shape
    return tensor.transpose(0, 2, 1, 3).reshape(tile_count * length, head_count, channels)


def causal(length):
    row_ids = lax.broadcasted_iota(jnp.int32, (length, length), 0)
    col_ids = lax.broadcasted_iota(jnp.int32, (length, length), 1)
    return row_ids >= col_ids


def reference(queries, key_rows, values, log_decays, output_grad):
    factor = DK ** -0.5
    scaled = to_blocks(queries, TILE_LEN) * factor
    keyed = to_blocks(key_rows, TILE_LEN)
    valued = to_blocks(values, TILE_LEN)
    cotangent = to_blocks(output_grad, TILE_LEN)
    cumulative = jnp.cumsum(to_blocks(log_decays, TILE_LEN), axis=2)
    lower_mask = causal(TILE_LEN)[None]
    head_count = queries.shape[1]

    def factors(local_cum):
        tile_total = local_cum[:, -1:, :]
        return jnp.exp(local_cum), jnp.exp(-local_cum), jnp.exp(tile_total - local_cum), jnp.exp(tile_total[:, 0, :])

    def forward_step(carried_over, inputs):
        query_tile, key_piece, value_piece, gradient_piece, local_cum = inputs
        growth, shrink, until_finish, piece_decay = factors(local_cum)
        scores = jnp.where(lower_mask, jnp.einsum("hiv,hjv->hij", gradient_piece, value_piece, precision=largest_entry), 0.0)
        local_part = jnp.einsum("hij,hjk->hik", scores, key_piece * shrink, precision=largest_entry)
        carried_portion = jnp.einsum("pge,pre->pgr", gradient_piece, carried_over, precision=largest_entry)
        refreshed_state = piece_decay[:, :, None] * carried_over + jnp.einsum("fnb,fne->fbe", key_piece * until_finish, value_piece, precision=largest_entry)
        return refreshed_state, growth * (local_part + carried_portion) * factor

    def backward_step(carried_over, inputs):
        query_tile, key_piece, value_piece, gradient_piece, local_cum = inputs
        growth, shrink, until_finish, piece_decay = factors(local_cum)
        amplified_query = query_tile * growth
        shrunk_key = key_piece * shrink
        attenuated_key = key_piece * until_finish
        scores = jnp.where(lower_mask, jnp.einsum("hiv,hjv->hij", gradient_piece, value_piece, precision=largest_entry), 0.0)
        key_local = shrink * jnp.einsum("hij,hik->hjk", scores, amplified_query, precision=largest_entry)
        key_passed_along = until_finish * jnp.einsum("ocb,orb->ocr", value_piece, carried_over, precision=largest_entry)
        weights = jnp.where(lower_mask, jnp.einsum("hik,hjk->hij", amplified_query, shrunk_key, precision=largest_entry), 0.0)
        value_local = jnp.einsum("hij,hiv->hjv", weights, gradient_piece, precision=largest_entry)
        value_passed_along = jnp.einsum("wbq,wqc->wbc", attenuated_key, carried_over, precision=largest_entry)
        refreshed_state = piece_decay[:, :, None] * carried_over + jnp.einsum("yaq,yao->yqo", amplified_query, gradient_piece, precision=largest_entry)
        return refreshed_state, (key_local + key_passed_along, value_local + value_passed_along)

    zero_state = jnp.zeros((head_count, DK, DV), jnp.float32)
    inputs = (scaled, keyed, valued, cotangent, cumulative)
    final_state, query_tiles = lax.scan(forward_step, zero_state, inputs)
    first_state, back_tiles = lax.scan(backward_step, zero_state, inputs, reverse=True)
    query_grad = from_blocks(query_tiles)
    key_grad = from_blocks(back_tiles[0])
    value_grad = from_blocks(back_tiles[1])
    position_grad = queries.astype(jnp.float32) * query_grad - key_rows.astype(jnp.float32) * key_grad
    decay_grad = jnp.flip(jnp.cumsum(jnp.flip(position_grad, 0), axis=0), 0)
    return query_grad, key_grad, value_grad, decay_grad
```

```python
import functools

import jax
import jax.numpy as jnp
from jax import lax
from jax.experimental import pallas as pl
from jax.experimental.pallas import tpu as pltpu
from jax.sharding import Mesh
from jax.sharding import PartitionSpec as P

DK = 128
SA = ("sa_0", "sa_1", "sa_2")
MESH = pl.DeviceIdType.MESH
F32, BF16 = jnp.float32, jnp.bfloat16
ROWS = 128
HALF = 64


def dot(a, b, dims):
    return lax.dot_general(a, b, (dims, ((), ())), preferred_element_type=F32)


NN, NT, TN = ((1,), (0,)), ((1,), (1,)), ((0,), (0,))


def split(x):
    hi = x.astype(BF16)
    return hi, (x - hi.astype(F32)).astype(BF16)


def both(x):
    hi, lo = split(x)
    return hi, jnp.concatenate([hi, lo], axis=0)


def folded(x):
    n = x.shape[0] // 2
    return x[:n] + x[n:]


def iotas(shape):
    return lax.broadcasted_iota(jnp.int32, shape, 0), lax.broadcasted_iota(jnp.int32, shape, 1)


def kernel(
    sizes,
    q_ref, k_ref, g_ref, v_ref, o_ref,
    dq_ref, dk_ref, dg_ref, dv_ref,
    vx, ox, qx, kx, gx,
    rloc, floc, lrow, lown,
    xr, xf, xl, xe,
    zsr, zsf, zr, zf, por, pof, cr, cf,
    sir, sif, rin, fin, da, db,
    ecum, eaft, dql, dkl, kend, dvl,
    early_s, early_r, p1_s, p1_r, p2_s, p2_r, p3_s, p3_r, p4_s, p4_r, fw_s, fw_r,
):
    ny, nz, nx = sizes
    np_ = ny * nz
    rp = ROWS // np_
    y, z, x = (lax.axis_index(name) for name in SA)
    a, b = lax.axis_index("ka"), lax.axis_index("vert")
    p = y * nz + z
    na, nb = 1 - a, 1 - b
    factor = DK ** (-0.5)

    def at_x(j):
        return (y, z, j, a, b)

    def at_p(j):
        return (j // nz, lax.rem(j, nz), x, a, b)

    def rdma(src, dst, ssem, rsem, dev):
        return pltpu.make_async_remote_copy(
            src_ref=src, dst_ref=dst, send_sem=ssem, recv_sem=rsem,
            device_id=dev, device_id_type=MESH,
        )

    barrier = pltpu.get_barrier_semaphore()
    for d in range(1, nx):
        pl.semaphore_signal(barrier, inc=1, device_id=at_x(lax.rem(x + d, nx)), device_id_type=MESH)

    def greet(d, carry):
        pl.semaphore_signal(
            barrier, inc=1, device_id=at_p(lax.rem(p + d, np_)), device_id_type=MESH
        )
        return carry

    lax.fori_loop(1, np_, greet, 0)
    for dev in ((y, z, x, a, nb), (y, z, x, na, b), (y, z, x, na, nb)):
        pl.semaphore_signal(barrier, inc=1, device_id=dev, device_id_type=MESH)

    jj, ii = iotas((ROWS, 4 * ROWS))
    col = lax.rem(ii, ROWS)
    kind = ii // ROWS
    upto = (jj <= col).astype(F32)
    first = (jj < ROWS // 2).astype(F32)
    sums = jnp.where(
        kind == 0, upto - first, jnp.where(kind == 1, upto, jnp.where(kind == 2, 1.0 - upto, 1.0))
    ).astype(BF16)
    ones8 = jnp.ones((8, ROWS), BF16)
    si, sj = iotas((ROWS, ROWS))
    lower = si >= sj

    pl.semaphore_wait(barrier, nx - 1 + np_ - 1 + 3)

    own8, oth8 = b * 8, nb * 8
    early = [
        rdma(o_ref.at[pl.ds(oth8, 8)], ox, early_s.at[0], early_r.at[0], (y, z, x, a, nb)),
        rdma(v_ref.at[pl.ds(oth8, 8)], vx, early_s.at[1], early_r.at[1], (y, z, x, a, nb)),
    ]
    oth512 = pl.multiple_of(na * 512, 512)
    for n, (src, dst) in enumerate(((q_ref, qx), (k_ref, kx), (g_ref, gx))):
        early.append(
            rdma(src.at[pl.ds(oth512, 512)], dst, early_s.at[2 + n], early_r.at[2 + n],
                 (y, z, x, na, b))
        )
    for copy in early:
        copy.start()

    def rows_of(h):
        return pl.ds(pl.multiple_of(h * HALF, HALF), HALF)

    def wide(own_ref, other, h):
        return jnp.concatenate([own_ref[own8 + h], other[h]], axis=1)

    def decays(h, carry):
        sums_h = dot(g_ref[rows_of(own8 + h)], sums, NN)
        r = rows_of(h)
        dql[r] = sums_h[:, :ROWS]
        ecum[r] = jnp.exp(sums_h[:, ROWS : 2 * ROWS])
        eaft[r] = jnp.exp(sums_h[:, 2 * ROWS : 3 * ROWS])
        lown[r] = sums_h[:, 3 * ROWS :]
        return carry

    lax.fori_loop(0, 8, decays, 0)
    for i in range(nx):
        lrow[i] = dot(ones8, g_ref[pl.ds(pl.multiple_of((own8 + 2 * i) * HALF, 128), 128)], NT)

    early[0].wait_recv()

    def p1(kind, i):
        src, dst = ((rloc, xr), (floc, xf), (lrow, xl))[kind]
        return rdma(src.at[i], dst.at[x], p1_s.at[kind, i], p1_r.at[kind, x], at_x(i))

    def p1_wait(kind, j):
        dst = (xr, xf, xl)[kind]
        rdma(dst.at[j], dst.at[j], p1_s.at[kind, j], p1_r.at[kind, j], at_x(j)).wait_recv()

    for i in range(nx):
        pl.when(i != x)(p1(2, i).start)

    def states(kind, i):
        for s in range(2):
            h = 2 * i + s
            r = rows_of(h)
            if kind == 0:
                left = q_ref[rows_of(own8 + h)].astype(F32) * factor * ecum[r]
                right = wide(o_ref, ox, h)
            else:
                left = k_ref[rows_of(own8 + h)].astype(F32) * eaft[r]
                right = wide(v_ref, vx, h)
            (rloc, floc)[kind][i, s * HALF : (s + 1) * HALF] = folded(dot(both(left)[1], right, NN))
        pl.when(i != x)(p1(kind, i).start)

    for i in range(nx):
        states(0, i)
    early[1].wait_recv()
    for i in range(nx):
        states(1, i)

    def local(h, carry):
        r = rows_of(h)
        rel = dql[r]
        grow, shrink = jnp.exp(rel), jnp.exp(-rel)
        scores = jnp.where(lower, dot(wide(o_ref, ox, h), wide(v_ref, vx, h), NT), 0.0)
        s_hi, s_lo = split(scores)
        k_hi, k_two = both(k_ref[rows_of(own8 + h)].astype(F32) * shrink)
        q_hi, q_two = both(q_ref[rows_of(own8 + h)].astype(F32) * factor * grow)
        dql[r] = (folded(dot(k_two, s_hi, NT)) + dot(k_hi, s_lo, NT)) * grow * factor
        dkl[r] = (folded(dot(q_two, s_hi, NN)) + dot(q_hi, s_lo, NN)) * shrink
        return carry

    lax.fori_loop(0, 8, local, 0)

    def widen(log_row):
        return jnp.exp(jnp.broadcast_to(log_row[0:1], (ROWS, ROWS)).T)

    def scaled(state, decay):
        return state * jnp.concatenate([decay, decay], axis=1)

    for j in range(nx):
        @pl.when(j == x)
        def _own():
            xr[j] = rloc[j]
            xf[j] = floc[j]
            xl[j] = lrow[j]

        @pl.when(j != x)
        def _wait():
            p1_wait(2, j)
            p1_wait(0, j)

        xe[j] = widen(xl[j])

    row_log = xl[0]
    for j in range(1, nx):
        row_log = row_log + xl[j]
    row_log = jnp.broadcast_to(row_log[0:1], (ROWS, ROWS)).T
    total = xr[nx - 1]
    for j in reversed(range(nx - 1)):
        total = scaled(total, xe[j]) + xr[j]
    zsr[:, :, : 2 * ROWS] = total.reshape(np_, rp, 2 * ROWS)
    zsr[:, :, 2 * ROWS :] = row_log.reshape(np_, rp, ROWS)

    def p2(kind, j):
        src, dst = ((zsr, zr), (zsf, zf))[kind]
        return rdma(src.at[j], dst.at[p], p2_s.at[kind, j], p2_r.at[kind, p], at_p(j))

    def p3(kind, j):
        src, dst = ((por, cr), (pof, cf))[kind]
        return rdma(src.at[j], dst.at[p], p3_s.at[kind, j], p3_r.at[kind, p], at_p(j))

    def to_all(make):
        def body(d, carry):
            make(lax.rem(p + d, np_)).start()
            return carry

        lax.fori_loop(1, np_, body, 0)

    def from_all(dst, ssem, rsem):
        def body(d, carry):
            j = lax.rem(p + d, np_)
            rdma(dst.at[j], dst.at[j], ssem.at[j], rsem.at[j], at_p(j)).wait_recv()
            return carry

        lax.fori_loop(1, np_, body, 0)

    to_all(functools.partial(p2, 0))
    zr[p] = zsr[p]

    for j in range(nx):
        @pl.when(j != x)
        def _wait():
            p1_wait(1, j)

    total = xf[0]
    for j in range(1, nx):
        total = scaled(total, xe[j]) + xf[j]
    zsf[...] = total.reshape(np_, rp, 2 * ROWS)
    to_all(functools.partial(p2, 1))
    zf[p] = zsf[p]

    for copy in early[2:]:
        copy.wait_recv()
    first_h = a * 8

    def value_local(h, carry):
        mine, theirs = rows_of(first_h + h), rows_of(h)
        g = jnp.concatenate([g_ref[mine], gx[theirs]], axis=0)
        sums_h = dot(g, sums[:, : 3 * ROWS], NN)
        rel = sums_h[:, :ROWS]
        qs = jnp.concatenate([q_ref[mine], qx[theirs]], axis=0).astype(F32) * factor
        ks = jnp.concatenate([k_ref[mine], kx[theirs]], axis=0).astype(F32)
        q_hi, q_lo = split(qs * jnp.exp(rel))
        k_hi, k_lo = split(ks * jnp.exp(-rel))
        kend[h] = ks * jnp.exp(sums_h[:, 2 * ROWS :])
        weights = dot(k_hi, q_hi, TN) + dot(k_hi, q_lo, TN) + dot(k_lo, q_hi, TN)
        weights = jnp.where(si <= sj, weights, 0.0)
        dvl[h] = folded(dot(both(weights)[1], o_ref[first_h + h], NN))
        return carry

    lax.fori_loop(0, 8, value_local, 0)

    from_all(zr, p2_s.at[0], p2_r.at[0])
    por[np_ - 1] = jnp.zeros((rp, 2 * ROWS), F32)
    run = zr[np_ - 1][:, : 2 * ROWS]
    for j in reversed(range(np_ - 1)):
        por[j] = run
        if j > 0:
            run = scaled(run, jnp.exp(zr[j][:, 2 * ROWS :])) + zr[j][:, : 2 * ROWS]
    to_all(functools.partial(p3, 0))
    cr[p] = por[p]

    from_all(zf, p2_s.at[1], p2_r.at[1])
    pof[0] = jnp.zeros((rp, 2 * ROWS), F32)
    run = zf[0]
    for j in range(1, np_):
        pof[j] = run
        if j < np_ - 1:
            run = scaled(run, jnp.exp(zr[j][:, 2 * ROWS :])) + zf[j]
    to_all(functools.partial(p3, 1))
    cf[p] = pof[p]

    def p4(kind, j):
        src, dst = ((sir, rin), (sif, fin))[kind]
        return rdma(src.at[j], dst.at[x], p4_s.at[kind, j], p4_r.at[kind, x], at_x(j))

    from_all(cr, p3_s.at[0], p3_r.at[0])
    run = cr[...].reshape(ROWS, 2 * ROWS)
    for j in reversed(range(nx)):
        sir[j] = run
        pl.when(j != x)(p4(0, j).start)
        if j > 0:
            run = scaled(run, xe[j]) + xr[j]
    rin[x] = sir[x]

    from_all(cf, p3_s.at[1], p3_r.at[1])
    run = cf[...].reshape(ROWS, 2 * ROWS)
    for j in range(nx):
        sif[j] = run
        pl.when(j != x)(p4(1, j).start)
        if j < nx - 1:
            run = scaled(run, xe[j]) + xf[j]
    fin[x] = sif[x]

    def lanes(half):
        return pl.ds(pl.multiple_of(half * ROWS, ROWS), ROWS)

    def forward(i, core):
        half = lax.rem(core + b, 2)
        return rdma(rin.at[i, :, lanes(half)], db.at[i], fw_s.at[core, i], fw_r.at[0, i],
                    (y, z, x, na, core))

    def across(i):
        return rdma(rin.at[i, :, lanes(1)], da.at[i], fw_s.at[0, i], fw_r.at[1, i],
                    (y, z, x, a, nb))

    def send_on(i):
        @pl.when(a != b)
        def _chip():
            forward(i, 0).start()
            forward(i, 1).start()

        @pl.when(a == b)
        def _core():
            across(i).start()

    for d in range(nx):
        j = lax.rem(x + d, nx)
        if d > 0:
            rdma(rin.at[j], rin.at[j], p4_s.at[0, j], p4_r.at[0, j], at_x(j)).wait_recv()
        send_on(j)

    def key_carried(h, carry):
        r = rows_of(h)
        state = rin[h // 2, rows_of(lax.rem(h, 2))]
        dkl[r] += folded(dot(both(state)[1], wide(v_ref, vx, h), NT)) * eaft[r]
        return carry

    lax.fori_loop(0, 8, key_carried, 0)

    for d in range(1, nx):
        j = lax.rem(x + d, nx)
        rdma(fin.at[j], fin.at[j], p4_s.at[1, j], p4_r.at[1, j], at_x(j)).wait_recv()

    later = (si >= sj).astype(BF16)

    def finish(h, carry):
        r = rows_of(h)
        i, sub = h // 2, rows_of(lax.rem(h, 2))
        state = fin[i, sub]
        dq = dql[r] + folded(dot(both(state)[1], wide(o_ref, ox, h), NT)) * ecum[r] * factor
        dk = dkl[r]
        dq_ref[r] = dq
        dk_ref[r] = dk
        final = scaled(state, jnp.exp(lown[r])) + floc[i, sub]
        beyond = jnp.sum(final * rin[i, sub], axis=1, keepdims=True)
        mine = rows_of(own8 + h)
        pos = q_ref[mine].astype(F32) * dq - k_ref[mine].astype(F32) * dk
        hi, mid = split(pos)
        low = (pos - hi.astype(F32) - mid.astype(F32)).astype(BF16)
        inside = dot(jnp.concatenate([hi, mid, low], axis=0), later, NN)
        dg_ref[r] = (inside[:HALF] + inside[HALF : 2 * HALF]) + inside[2 * HALF :] + beyond
        return carry

    lax.fori_loop(0, 8, finish, 0)

    for i in range(nx):
        rdma(db.at[i], db.at[i], fw_s.at[0, i], fw_r.at[0, i], (y, z, x, na, b)).wait_recv()

        @pl.when(a != b)
        def _take():
            rdma(da.at[i], da.at[i], fw_s.at[0, i], fw_r.at[1, i], (y, z, x, a, nb)).wait_recv()

        @pl.when(a == b)
        def _copy():
            da[i] = rin[i, :, :ROWS]

    def value_finish(h, carry):
        i, sub = h // 2, rows_of(lax.rem(h, 2))
        s_hi, s_lo = split(jnp.concatenate([da[i, sub], db[i, sub]], axis=0))
        k_hi, k_lo = split(kend[h])
        dv_ref[h] = dvl[h] + dot(k_hi, s_hi, TN) + dot(k_hi, s_lo, TN) + dot(k_lo, s_hi, TN)
        return carry

    lax.fori_loop(0, 8, value_finish, 0)

    for copy in early:
        copy.wait_send()
    for i in range(nx):
        @pl.when(i != x)
        def _sent():
            for kind in range(3):
                p1(kind, i).wait_send()
            for kind in range(2):
                p4(kind, i).wait_send()

        @pl.when(a != b)
        def _sent_chip():
            forward(i, 0).wait_send()
            forward(i, 1).wait_send()

        @pl.when(a == b)
        def _sent_core():
            across(i).wait_send()

    def sent(d, carry):
        j = lax.rem(p + d, np_)
        for kind in range(2):
            p2(kind, j).wait_send()
            p3(kind, j).wait_send()
        return carry

    lax.fori_loop(1, np_, sent, 0)


def shards(sizes, queries, key_rows, values, log_decays, output_grad):
    ny, nz, nx = sizes
    np_ = ny * nz
    rp = ROWS // np_
    qt, kt, gt = (t.transpose(1, 2, 0).reshape(-1, ROWS) for t in (queries, key_rows, log_decays))
    vh, oh = (t.transpose(1, 0, 2) for t in (values, output_grad))
    vmem = pl.BlockSpec(memory_space=pltpu.VMEM)
    dma = pltpu.SemaphoreType.DMA

    def f32(*shape):
        return pltpu.VMEM(shape, F32)

    def bf16(*shape):
        return pltpu.VMEM(shape, BF16)

    sq, state = (ROWS, ROWS), (ROWS, 2 * ROWS)
    dq, dk, dg, dv = pl.pallas_call(
        functools.partial(kernel, sizes),
        out_shape=[jax.ShapeDtypeStruct((512, ROWS), F32)] * 3
        + [jax.ShapeDtypeStruct((8, ROWS, ROWS), F32)],
        in_specs=[vmem] * 5,
        out_specs=[vmem] * 4,
        scratch_shapes=[bf16(8, *sq)] * 2 + [bf16(512, ROWS)] * 3
        + [f32(nx, *state)] * 2 + [f32(nx, 8, ROWS), f32(512, ROWS)]
        + [f32(nx, *state)] * 2 + [f32(nx, 8, ROWS), f32(nx, *sq)]
        + [f32(np_, rp, 3 * ROWS), f32(np_, rp, 2 * ROWS)] * 2
        + [f32(np_, rp, 2 * ROWS)] * 4
        + [f32(nx, *state)] * 4 + [f32(nx, *sq)] * 2
        + [f32(512, ROWS)] * 4 + [f32(8, *sq)] * 2
        + [dma((5,))] * 2 + [dma((3, nx))] * 2 + [dma((2, np_))] * 4
        + [dma((2, nx))] * 4,
        compiler_params=pltpu.CompilerParams(collective_id=0, has_side_effects=True),
    )(qt, kt, gt, vh, oh)
    dq, dk, dg = (t.reshape(8, HALF, ROWS).transpose(2, 0, 1) for t in (dq, dk, dg))
    return dq, dk, dv.transpose(1, 0, 2), dg


def solution(mesh):
    ka, vert = mesh.shape["ka"], mesh.shape["vert"]
    sizes = (2, 8, 4)
    if mesh.shape["sa"] != 64:
        sizes = (mesh.shape["sa"] // 4, 1, 4)
    finer = Mesh(mesh.devices.reshape(*sizes, ka, vert), (*SA, "ka", "vert"))
    return jax.shard_map(
        functools.partial(shards, sizes),
        mesh=finer,
        in_specs=(P(SA, None, "ka"),) * 2 + (P(SA, None, "vert"), P(SA, None, "ka"), P(SA, None, "vert")),
        out_specs=(P(SA, "vert", "ka"), P(SA, "vert", "ka"), P(SA, "ka", "vert"), P(SA, "vert", "ka")),
        check_vma=False,
    )
```
